8 devices in a mesh: dp: 1 (over z), tp: 8 (over x, y, core).
Axes of the slice: x: 2, y: 2, z: 1, core: 2. Of those that a mesh axis runs over, the one named last changes fastest.
Arguments:
- x: bfloat16 [768, 12288], P(('dp', 'tp'))
- w_gate: bfloat16 [12288, 33792], P(None, 'tp')
- w_up: bfloat16 [12288, 33792], P(None, 'tp')
- w_down: bfloat16 [33792, 12288], P('tp')
Outputs:
- output: bfloat16 [768, 12288], P(('dp', 'tp'))
All inputs are finite; a program needn't handle non-finite values.
Results may differ from the reference program's by a relative error of at most 0.016.
Values are sent between devices in bfloat16 or wider.
A program may use at most 2 GiB of HBM per device.

```python
import jax
import jax.numpy as jnp

ROWS = 768
D = 12288
FF = 33792


def setup_inputs(seed: int = 0, part: int = 0) -> dict:
    kx, kg, ku, kd = jax.random.split(jax.random.key(seed), 4)
    drawn = {
        "x": jax.random.normal(jax.random.fold_in(kx, part), (ROWS, D), jnp.float32),
        "w_gate": jax.random.normal(kg, (D, FF), jnp.float32) * D**-0.5,
        "w_up": jax.random.normal(ku, (D, FF), jnp.float32) * D**-0.5,
        "w_down": jax.random.normal(kd, (FF, D), jnp.float32) * FF**-0.5,
    }
    return {k: v.astype(jnp.bfloat16) for k, v in drawn.items()}


def reference(x, w_gate, w_up, w_down):
    gate = jnp.dot(x, w_gate, preferred_element_type=jnp.float32)
    up = jnp.dot(x, w_up, preferred_element_type=jnp.float32)
    hidden = (jax.nn.silu(gate) * up).astype(jnp.bfloat16)
    return jnp.dot(hidden, w_down, preferred_element_type=jnp.float32).astype(jnp.bfloat16)
```

```python
import jax
import jax.numpy as jnp
from jax import lax
from jax.experimental import pallas as pl
from jax.experimental.pallas import tpu as pltpu
from jax.sharding import PartitionSpec as P

BF, F32 = jnp.bfloat16, jnp.float32
KC = 768
NB = 1408
NC = 512
VMEM = 67_000_000

SENDS = ((0, 1, 0), (0, 2, 1), (0, 4, 2), (2, 3, 0), (1, 5, 2), (2, 6, 2), (3, 7, 2))


def neighbours():
    me = lax.axis_index("tp")
    core, y, x = me % 2, (me // 2) % 2, me // 4
    over_x, over_y = me + 4 * (1 - 2 * x), me + 2 * (1 - 2 * y)
    a = over_x * (1 - core) + over_y * core
    b = over_x * core + over_y * (1 - core)
    return a, b, me + 1 - 2 * core


def greet(others):
    barrier = pltpu.get_barrier_semaphore()
    for other in others:
        pl.semaphore_signal(barrier, inc=1, device_id={"tp": other}, device_id_type=pl.DeviceIdType.MESH)
    pl.semaphore_wait(barrier, len(others))


def gather_up(x_ref, wg_ref, wu_ref, h_ref, xg, acc, wbuf, hbuf, lsem, ssem, rsem, wsem, hsem):
    rows = x_ref.shape[0]
    nk, nb, slots = xg.shape[0], acc.shape[0], wbuf.shape[0]
    total = nk * nb
    others = neighbours()

    def local(c):
        k0 = pl.multiple_of(c * KC, KC)
        return pltpu.make_async_copy(x_ref.at[:, pl.ds(k0, KC)], xg.at[c, pl.ds(0, rows)], lsem.at[c])

    def remote(kind, c):
        src, dst, to = SENDS[kind]
        return pltpu.make_async_remote_copy(
            src_ref=xg.at[c, pl.ds(src * rows, rows)],
            dst_ref=xg.at[c, pl.ds(dst * rows, rows)],
            send_sem=ssem.at[kind, c],
            recv_sem=rsem.at[kind, c],
            device_id={"tp": others[to]},
            device_id_type=pl.DeviceIdType.MESH,
        )

    def weights(s):
        k0, n0 = pl.multiple_of((s // nb) * KC, KC), pl.multiple_of((s % nb) * NB, 128)
        slot = s % slots
        return [
            pltpu.make_async_copy(
                w.at[pl.ds(k0, KC), pl.ds(n0, NB)], wbuf.at[slot, :, pl.ds(i * NB, NB)], wsem.at[slot, i]
            )
            for i, w in enumerate((wg_ref, wu_ref))
        ]

    def start(copies):
        for copy in copies:
            copy.start()

    def wait(copies):
        for copy in copies:
            copy.wait()

    def own(c):
        local(c).wait()
        for kind in (0, 1, 2):
            remote(kind, c).start()

    def pass_on(c):
        remote(1, c).wait_recv()
        remote(3, c).start()
        remote(5, c).start()
        remote(0, c).wait_recv()
        remote(4, c).start()

    def pass_far(c):
        remote(3, c).wait_recv()
        remote(6, c).start()

    def ready(c):
        for kind in (2, 4, 5, 6):
            remote(kind, c).wait_recv()

    local(0).start()
    start(weights(0))

    @pl.loop(1, nk)
    def _(c):
        local(c).start()

    for s in range(1, slots - 1):
        start(weights(s))
    greet(others)
    own(0)

    @pl.loop(0, nb)
    def _(n):
        @pl.loop(0, acc.shape[1] // 32)
        def _(r):
            acc[n, pl.ds(pl.multiple_of(r * 32, 32), 32), :] = jnp.zeros((32, 2 * NB), F32)

    pass_on(0)
    own(1)
    pass_far(0)

    def dot(c, s, n):
        acc[n] += jnp.dot(xg[c], wbuf[s % slots], preferred_element_type=F32)

    @pl.loop(0, total - nb)
    def _(s):
        c, n = s // nb, s % nb

        @pl.when(n == 0)
        def _():
            ready(c)

            @pl.when(c + 2 < nk)
            def _():
                own(c + 2)

        @pl.when(n == 1)
        def _():
            @pl.when(c == 0)
            def _():
                pass_on(1)

            @pl.when(c > 0)
            def _():
                pass_far(c + 1)

        @pl.when(n == 2)
        def _():
            @pl.when(c == 0)
            def _():
                pass_far(1)

            @pl.when(c + 2 < nk)
            def _():
                pass_on(c + 2)

        @pl.when(s + slots - 1 < total)
        def _():
            start(weights(s + slots - 1))

        wait(weights(s))
        dot(c, s, n)

    def put(n):
        return pltpu.make_async_copy(hbuf.at[n % 2], h_ref.at[:, pl.ds(n * NB, NB)], hsem.at[n % 2])

    def hide(n):
        for r in range(0, acc.shape[1], 16):
            gate, up = acc[n, r : r + 16, :NB], acc[n, r : r + 16, NB:]
            hbuf[n % 2, r : r + 16] = (jax.nn.silu(gate) * up).astype(BF)

    ready(nk - 1)
    for n in range(nb):
        s = total - nb + n
        if s + slots - 1 < total:
            start(weights(s + slots - 1))
        wait(weights(s))
        if n >= 3:
            put(n - 3).wait()
        if n >= 1:
            hide(n - 1)
        dot(nk - 1, s, n)
        if n >= 1:
            put(n - 1).start()
    if nb >= 3:
        put(nb - 3).wait()
    hide(nb - 1)
    put(nb - 1).start()
    put(nb - 2).wait()
    put(nb - 1).wait()

    @pl.loop(0, nk)
    def _(c):
        for kind in range(len(SENDS)):
            remote(kind, c).wait_send()


LAG = (2, 5, 8)
FREE = 8


def down_scatter(
    h_ref, wd_ref, y_ref, hid, wbuf, own, kept, part, yout, out_p, in_p, out_a, in_a, out_b, in_b,
    hsem, wsem, ysem, sems_p, sems_a, sems_b,
):
    rows = y_ref.shape[0]
    slots = wbuf.shape[0]
    count = y_ref.shape[1] // NC
    others = neighbours()

    def weights(i):
        n0 = pl.multiple_of(i * NC, NC)
        return pltpu.make_async_copy(wd_ref.at[:, pl.ds(n0, NC)], wbuf.at[i % slots], wsem.at[i % slots])

    def remote(i, out, into, sems, to):
        return pltpu.make_async_remote_copy(
            src_ref=out.at[i % 4],
            dst_ref=into.at[i + FREE],
            send_sem=sems.at[0, i],
            recv_sem=sems.at[1, i],
            device_id={"tp": others[to]},
            device_id_type=pl.DeviceIdType.MESH,
        )

    def to_p(i):
        return remote(i, out_p, in_p, sems_p, 2)

    def to_a(i):
        return remote(i, out_a, in_a, sems_a, 0)

    def to_b(i):
        return remote(i, out_b, in_b, sems_b, 1)

    def result(i):
        n0 = pl.multiple_of(i * NC, NC)
        return pltpu.make_async_copy(yout.at[i % 4], y_ref.at[:, pl.ds(n0, NC)], ysem.at[i % 4])

    def pair_sum(i):
        there = in_p[i + FREE]
        mine, slot = own.at[(i + FREE) % 4], (i + FREE) % 4
        out = out_a.at[slot]
        kept[(i + FREE) % 8, :rows] = mine[:rows] + there[:rows].astype(F32)
        kept[(i + FREE) % 8, rows:] = mine[2 * rows : 3 * rows] + there[2 * rows : 3 * rows].astype(F32)
        out[:rows] = (mine[rows : 2 * rows] + there[rows : 2 * rows].astype(F32)).astype(BF)
        out[rows:] = (mine[3 * rows :] + there[3 * rows :].astype(F32)).astype(BF)

    def next_sum(i):
        there = in_a[i + FREE]
        slot = (i + FREE) % 8
        part[slot] = kept[slot, :rows] + there[:rows].astype(F32)
        out_b[(i + FREE) % 4] = (kept[slot, rows:] + there[rows:].astype(F32)).astype(BF)

    def last_sum(i):
        yout[(i + FREE) % 4] = (part[(i + FREE) % 8] + in_b[i + FREE].astype(F32)).astype(BF)

    whole = pltpu.make_async_copy(h_ref, hid, hsem)
    whole.start()
    for i in range(slots - 1):
        weights(i).start()
    greet(others)
    whole.wait()

    @pl.loop(0, count)
    def _(i):
        @pl.when(i + slots - 1 < count)
        def _():
            weights(i + slots - 1).start()

        weights(i).wait()

        @pl.when(i >= 4)
        def _():
            to_p(i - 4).wait_send()

        @pl.when(i >= LAG[0])
        def _():
            to_p(i - LAG[0]).wait_recv()

        @pl.when(i >= LAG[0] + 4)
        def _():
            to_a(i - LAG[0] - 4).wait_send()

        @pl.when(i >= LAG[1])
        def _():
            to_a(i - LAG[1]).wait_recv()

        @pl.when(i >= LAG[1] + 4)
        def _():
            to_b(i - LAG[1] - 4).wait_send()

        @pl.when(i >= LAG[2])
        def _():
            to_b(i - LAG[2]).wait_recv()

        @pl.when(i >= LAG[2] + 4)
        def _():
            result(i - LAG[2] - 4).wait()

        last_sum(i - LAG[2])
        next_sum(i - LAG[1])
        pair_sum(i - LAG[0])
        term = jnp.dot(hid[...], wbuf[i % slots], preferred_element_type=F32)
        out_p[i % 4] = term[4 * rows :].astype(BF)
        own[i % 4] = term[: 4 * rows]

        @pl.when(i >= LAG[1])
        def _():
            to_b(i - LAG[1]).start()

        @pl.when(i >= LAG[0])
        def _():
            to_a(i - LAG[0]).start()

        @pl.when(i >= LAG[2])
        def _():
            result(i - LAG[2]).start()

        to_p(i).start()

    for i in range(count, count + LAG[2]):
        if i - LAG[0] < count:
            to_p(i - LAG[0]).wait_recv()
            to_a(i - LAG[0] - 4).wait_send()
            pair_sum(i - LAG[0])
            to_a(i - LAG[0]).start()
        if i - LAG[1] < count:
            to_a(i - LAG[1]).wait_recv()
            to_b(i - LAG[1] - 4).wait_send()
            next_sum(i - LAG[1])
            to_b(i - LAG[1]).start()
        to_b(i - LAG[2]).wait_recv()
        result(i - LAG[2] - 4).wait()
        last_sum(i - LAG[2])
        result(i - LAG[2]).start()
    for i in range(count - 4, count):
        to_p(i).wait_send()
        to_a(i).wait_send()
        to_b(i).wait_send()
        result(i).wait()


def solution(mesh):
    def step(x, w_gate, w_up, w_down):
        (rows, width), units = x.shape, w_gate.shape[1]
        tokens = rows * mesh.shape["tp"]
        nk, nb, count = width // KC, units // NB, width // NC
        dma = pltpu.SemaphoreType.DMA
        anywhere = pl.BlockSpec(memory_space=pl.ANY)
        h = pl.pallas_call(
            gather_up,
            out_shape=jax.ShapeDtypeStruct((tokens, units), BF),
            in_specs=[anywhere] * 3,
            out_specs=anywhere,
            scratch_shapes=[
                pltpu.VMEM((nk, tokens, KC), BF),
                pltpu.VMEM((nb, tokens, 2 * NB), F32),
                pltpu.VMEM((2, KC, 2 * NB), BF),
                pltpu.VMEM((2, tokens, NB), BF),
                dma((nk,)),
                dma((len(SENDS), nk)),
                dma((len(SENDS), nk)),
                dma((2, 2)),
                dma((2,)),
            ],
            compiler_params=pltpu.CompilerParams(collective_id=0, has_side_effects=True, vmem_limit_bytes=VMEM),
            name="gather_up",
        )(x, w_gate, w_up)
        return pl.pallas_call(
            down_scatter,
            out_shape=jax.ShapeDtypeStruct((rows, width), BF),
            in_specs=[anywhere] * 2,
            out_specs=anywhere,
            scratch_shapes=[
                pltpu.VMEM((tokens, units), BF),
                pltpu.VMEM((3, units, NC), BF),
                pltpu.VMEM((4, 4 * rows, NC), F32),
                pltpu.VMEM((8, 2 * rows, NC), F32),
                pltpu.VMEM((8, rows, NC), F32),
                pltpu.VMEM((4, rows, NC), BF),
                pltpu.VMEM((4, 4 * rows, NC), BF),
                pltpu.VMEM((count + FREE, 4 * rows, NC), BF),
                pltpu.VMEM((4, 2 * rows, NC), BF),
                pltpu.VMEM((count + FREE, 2 * rows, NC), BF),
                pltpu.VMEM((4, rows, NC), BF),
                pltpu.VMEM((count + FREE, rows, NC), BF),
                dma,
                dma((3,)),
                dma((4,)),
                dma((2, count)),
                dma((2, count)),
                dma((2, count)),
            ],
            compiler_params=pltpu.CompilerParams(collective_id=1, has_side_effects=True, vmem_limit_bytes=VMEM),
            name="down_scatter",
        )(h, w_down)

    return jax.shard_map(
        step,
        mesh=mesh,
        in_specs=(P(("dp", "tp"), None), P(None, "tp"), P(None, "tp"), P("tp", None)),
        out_specs=P(("dp", "tp"), None),
        check_vma=False,
    )
```

```python
import jax
import jax.numpy as jnp
from jax import lax
from jax.experimental import pallas as pl
from jax.experimental.pallas import tpu as pltpu
from jax.sharding import PartitionSpec as P

BF, F32 = jnp.bfloat16, jnp.float32
KC = 1024
NB = 1408
PIECES = 4
NC = 512
VMEM = 67_000_000

SENDS = ((0, 1, 0), (0, 2, 1), (0, 4, 2), (2, 3, 0), (1, 5, 2), (2, 6, 2), (3, 7, 2))


def neighbours():
    me = lax.axis_index("tp")
    core, y, x = me % 2, (me // 2) % 2, me // 4
    over_x, over_y = me + 4 * (1 - 2 * x), me + 2 * (1 - 2 * y)
    a = over_x * (1 - core) + over_y * core
    b = over_x * core + over_y * (1 - core)
    return a, b, me + 1 - 2 * core


def greet(others):
    barrier = pltpu.get_barrier_semaphore()
    for other in others:
        pl.semaphore_signal(barrier, inc=1, device_id={"tp": other}, device_id_type=pl.DeviceIdType.MESH)
    pl.semaphore_wait(barrier, len(others))


def gather_up(x_ref, wg_ref, wu_ref, h_ref, xg, acc, wbuf, lsem, ssem, rsem, fssem, frsem, wsem, hsem):
    rows = x_ref.shape[0]
    nk, nb, slots = xg.shape[0], acc.shape[0], wbuf.shape[0]
    total = nk * nb
    others = neighbours()

    def local(c):
        k0 = pl.multiple_of(c * KC, KC)
        return pltpu.make_async_copy(x_ref.at[:, pl.ds(k0, KC)], xg.at[c, pl.ds(0, rows)], lsem.at[c])

    def remote(kind, c):
        src, dst, to = SENDS[kind]
        return pltpu.make_async_remote_copy(
            src_ref=xg.at[c, pl.ds(src * rows, rows)],
            dst_ref=xg.at[c, pl.ds(dst * rows, rows)],
            send_sem=ssem.at[kind, c],
            recv_sem=rsem.at[kind, c],
            device_id={"tp": others[to]},
            device_id_type=pl.DeviceIdType.MESH,
        )

    def first(kind, piece):
        src, dst, to = SENDS[kind]
        columns = pl.ds(piece * (KC // PIECES), KC // PIECES)
        return pltpu.make_async_remote_copy(
            src_ref=xg.at[0, pl.ds(src * rows, rows), columns],
            dst_ref=xg.at[0, pl.ds(dst * rows, rows), columns],
            send_sem=fssem.at[kind, piece],
            recv_sem=frsem.at[kind, piece],
            device_id={"tp": others[to]},
            device_id_type=pl.DeviceIdType.MESH,
        )

    def weights(s):
        k0, n0 = pl.multiple_of((s // nb) * KC, KC), pl.multiple_of((s % nb) * NB, 128)
        slot = s % slots
        return [
            pltpu.make_async_copy(
                w.at[pl.ds(k0, KC), pl.ds(n0, NB)], wbuf.at[slot, :, pl.ds(i * NB, NB)], wsem.at[slot, i]
            )
            for i, w in enumerate((wg_ref, wu_ref))
        ]

    def start(copies):
        for copy in copies:
            copy.start()

    def wait(copies):
        for copy in copies:
            copy.wait()

    def own(c):
        local(c).wait()
        for kind in (0, 1, 2):
            remote(kind, c).start()

    def pass_on(c):
        remote(1, c).wait_recv()
        remote(3, c).start()
        remote(5, c).start()
        remote(0, c).wait_recv()
        remote(4, c).start()

    def pass_far(c):
        remote(3, c).wait_recv()
        remote(6, c).start()

    def ready(c):
        for kind in (2, 4, 5, 6):
            remote(kind, c).wait_recv()

    local(0).start()
    start(weights(0))

    @pl.loop(1, nk)
    def _(c):
        local(c).start()

    for s in range(1, slots - 1):
        start(weights(s))
    greet(others)
    local(0).wait()
    for piece in range(PIECES):
        for kind in (0, 1, 2):
            first(kind, piece).start()

    @pl.loop(0, nb)
    def _(n):
        @pl.loop(0, acc.shape[1] // 32)
        def _(r):
            acc[n, pl.ds(pl.multiple_of(r * 32, 32), 32), :] = jnp.zeros((32, 2 * NB), F32)

    for piece in range(PIECES):
        first(1, piece).wait_recv()
        first(3, piece).start()
        first(5, piece).start()
        first(0, piece).wait_recv()
        first(4, piece).start()
    for piece in range(PIECES):
        if piece == PIECES - 1:
            own(1)
        first(3, piece).wait_recv()
        first(6, piece).start()
    for piece in range(PIECES):
        for kind in (2, 4, 5, 6):
            first(kind, piece).wait_recv()

    def dot(c, s, n):
        acc[n] += jnp.dot(xg[c], wbuf[s % slots], preferred_element_type=F32)

    @pl.loop(0, total - nb)
    def _(s):
        c, n = s // nb, s % nb

        @pl.when(n == 0)
        def _():
            @pl.when(c > 0)
            def _():
                ready(c)

            @pl.when(c + 2 < nk)
            def _():
                own(c + 2)

        @pl.when(n == 1)
        def _():
            @pl.when(c == 0)
            def _():
                pass_on(1)

            @pl.when(c > 0)
            def _():
                pass_far(c + 1)

        @pl.when(n == 2)
        def _():
            @pl.when(c == 0)
            def _():
                pass_far(1)

            @pl.when(c + 2 < nk)
            def _():
                pass_on(c + 2)

        @pl.when(s + slots - 1 < total)
        def _():
            start(weights(s + slots - 1))

        wait(weights(s))
        dot(c, s, n)

    def put(n):
        return [
            pltpu.make_async_copy(xg.at[2 * n], h_ref.at[:, pl.ds(n * NB, KC)], hsem.at[n, 0]),
            pltpu.make_async_copy(
                xg.at[2 * n + 1, :, pl.ds(0, NB - KC)], h_ref.at[:, pl.ds(n * NB + KC, NB - KC)], hsem.at[n, 1]
            ),
        ]

    def hide(n):
        for r in range(0, acc.shape[1], 16):
            gate, up = acc[n, r : r + 16, :NB], acc[n, r : r + 16, NB:]
            hidden = (jax.nn.silu(gate) * up).astype(BF)
            xg[2 * n, r : r + 16] = hidden[:, :KC]
            xg[2 * n + 1, r : r + 16, : NB - KC] = hidden[:, KC:]

    for piece in range(PIECES):
        for kind in range(len(SENDS)):
            first(kind, piece).wait_send()

    @pl.loop(1, nk)
    def _(c):
        for kind in range(len(SENDS)):
            remote(kind, c).wait_send()

    ready(nk - 1)
    for n in range(nb):
        s = total - nb + n
        if s + slots - 1 < total:
            start(weights(s + slots - 1))
        wait(weights(s))
        if n >= 1:
            hide(n - 1)
        dot(nk - 1, s, n)
        if n >= 1:
            start(put(n - 1))
    hide(nb - 1)
    start(put(nb - 1))
    for n in range(nb):
        wait(put(n))


LAG = (1, 3, 5)
FREE = 8


def down_scatter(
    h_ref, wd_ref, y_ref, hid, wbuf, own, kept, part, yout, out_p, in_p, out_a, in_a, out_b, in_b,
    hsem, wsem, ysem, sems_p, sems_a, sems_b,
):
    rows = y_ref.shape[0]
    slots = wbuf.shape[0]
    count = y_ref.shape[1] // NC
    others = neighbours()

    def weights(i):
        n0 = pl.multiple_of(i * NC, NC)
        return pltpu.make_async_copy(wd_ref.at[:, pl.ds(n0, NC)], wbuf.at[i % slots], wsem.at[i % slots])

    def remote(i, out, into, sems, to):
        return pltpu.make_async_remote_copy(
            src_ref=out.at[i % 4],
            dst_ref=into.at[i + FREE],
            send_sem=sems.at[0, i],
            recv_sem=sems.at[1, i],
            device_id={"tp": others[to]},
            device_id_type=pl.DeviceIdType.MESH,
        )

    def to_p(i):
        return remote(i, out_p, in_p, sems_p, 2)

    def to_a(i):
        return remote(i, out_a, in_a, sems_a, 0)

    def to_b(i):
        return remote(i, out_b, in_b, sems_b, 1)

    def result(i):
        n0 = pl.multiple_of(i * NC, NC)
        return pltpu.make_async_copy(yout.at[i % 4], y_ref.at[:, pl.ds(n0, NC)], ysem.at[i % 4])

    def pair_sum(i):
        there = in_p[i + FREE]
        mine, slot = own.at[(i + FREE) % 4], (i + FREE) % 4
        out = out_a.at[slot]
        kept[(i + FREE) % 8, :rows] = mine[:rows] + there[:rows].astype(F32)
        kept[(i + FREE) % 8, rows:] = mine[2 * rows : 3 * rows] + there[2 * rows : 3 * rows].astype(F32)
        out[:rows] = (mine[rows : 2 * rows] + there[rows : 2 * rows].astype(F32)).astype(BF)
        out[rows:] = (mine[3 * rows :] + there[3 * rows :].astype(F32)).astype(BF)

    def next_sum(i):
        there = in_a[i + FREE]
        slot = (i + FREE) % 8
        part[slot] = kept[slot, :rows] + there[:rows].astype(F32)
        out_b[(i + FREE) % 4] = (kept[slot, rows:] + there[rows:].astype(F32)).astype(BF)

    def last_sum(i):
        yout[(i + FREE) % 4] = (part[(i + FREE) % 8] + in_b[i + FREE].astype(F32)).astype(BF)

    whole = pltpu.make_async_copy(h_ref, hid, hsem)
    whole.start()
    for i in range(slots - 1):
        weights(i).start()
    greet(others)
    whole.wait()

    def waits(i):
        @pl.when(i + slots - 1 < count)
        def _():
            weights(i + slots - 1).start()

        weights(i).wait()

        @pl.when(i >= 4)
        def _():
            to_p(i - 4).wait_send()

        @pl.when(i >= LAG[0])
        def _():
            to_p(i - LAG[0]).wait_recv()

        @pl.when(i >= LAG[0] + 4)
        def _():
            to_a(i - LAG[0] - 4).wait_send()

        @pl.when(i >= LAG[1])
        def _():
            to_a(i - LAG[1]).wait_recv()

        @pl.when(i >= LAG[1] + 4)
        def _():
            to_b(i - LAG[1] - 4).wait_send()

        @pl.when(i >= LAG[2])
        def _():
            to_b(i - LAG[2]).wait_recv()

        @pl.when(i >= LAG[2] + 4)
        def _():
            result(i - LAG[2] - 4).wait()

    def compute(i, summed, passed):
        last_sum(i - LAG[2])
        next_sum(i - LAG[1])
        pair_sum(i - LAG[0])
        w = wbuf.at[i % slots]
        out_p[i % 4] = jnp.dot(hid[4 * rows :], w[...], preferred_element_type=F32).astype(BF)
        if passed:
            to_b(i - LAG[1]).start()
        if summed:
            to_a(i - LAG[0]).start()
        to_p(i).start()
        own[i % 4] = jnp.dot(hid[: 4 * rows], w[...], preferred_element_type=F32)

    for i in range(LAG[1]):
        waits(i)
        compute(i, i >= LAG[0], False)

    @pl.loop(LAG[1], count)
    def _(i):
        waits(i)
        compute(i, True, True)

        @pl.when(i >= LAG[2])
        def _():
            result(i - LAG[2]).start()

    for i in range(count, count + LAG[2]):
        if i - LAG[0] < count:
            to_p(i - LAG[0]).wait_recv()
            to_a(i - LAG[0] - 4).wait_send()
            pair_sum(i - LAG[0])
            to_a(i - LAG[0]).start()
        if i - LAG[1] < count:
            to_a(i - LAG[1]).wait_recv()
            to_b(i - LAG[1] - 4).wait_send()
            next_sum(i - LAG[1])
            to_b(i - LAG[1]).start()
        to_b(i - LAG[2]).wait_recv()
        result(i - LAG[2] - 4).wait()
        last_sum(i - LAG[2])
        result(i - LAG[2]).start()
    for i in range(count - 4, count):
        to_p(i).wait_send()
        to_a(i).wait_send()
        to_b(i).wait_send()
        result(i).wait()


def solution(mesh):
    def step(x, w_gate, w_up, w_down):
        (rows, width), units = x.shape, w_gate.shape[1]
        tokens = rows * mesh.shape["tp"]
        nk, nb, count = width // KC, units // NB, width // NC
        dma = pltpu.SemaphoreType.DMA
        anywhere = pl.BlockSpec(memory_space=pl.ANY)
        h = pl.pallas_call(
            gather_up,
            out_shape=jax.ShapeDtypeStruct((tokens, units), BF),
            in_specs=[anywhere] * 3,
            out_specs=anywhere,
            scratch_shapes=[
                pltpu.VMEM((nk, tokens, KC), BF),
                pltpu.VMEM((nb, tokens, 2 * NB), F32),
                pltpu.VMEM((2, KC, 2 * NB), BF),
                dma((nk,)),
                dma((len(SENDS), nk)),
                dma((len(SENDS), nk)),
                dma((len(SENDS), PIECES)),
                dma((len(SENDS), PIECES)),
                dma((2, 2)),
                dma((nb, 2)),
            ],
            compiler_params=pltpu.CompilerParams(collective_id=0, has_side_effects=True, vmem_limit_bytes=VMEM),
            name="gather_up",
        )(x, w_gate, w_up)
        return pl.pallas_call(
            down_scatter,
            out_shape=jax.ShapeDtypeStruct((rows, width), BF),
            in_specs=[anywhere] * 2,
            out_specs=anywhere,
            scratch_shapes=[
                pltpu.VMEM((tokens, units), BF),
                pltpu.VMEM((3, units, NC), BF),
                pltpu.VMEM((4, 4 * rows, NC), F32),
                pltpu.VMEM((8, 2 * rows, NC), F32),
                pltpu.VMEM((8, rows, NC), F32),
                pltpu.VMEM((4, rows, NC), BF),
                pltpu.VMEM((4, 4 * rows, NC), BF),
                pltpu.VMEM((count + FREE, 4 * rows, NC), BF),
                pltpu.VMEM((4, 2 * rows, NC), BF),
                pltpu.VMEM((count + FREE, 2 * rows, NC), BF),
                pltpu.VMEM((4, rows, NC), BF),
                pltpu.VMEM((count + FREE, rows, NC), BF),
                dma,
                dma((3,)),
                dma((4,)),
                dma((2, count)),
                dma((2, count)),
                dma((2, count)),
            ],
            compiler_params=pltpu.CompilerParams(collective_id=1, has_side_effects=True, vmem_limit_bytes=VMEM),
            name="down_scatter",
        )(h, w_down)

    return jax.shard_map(
        step,
        mesh=mesh,
        in_specs=(P(("dp", "tp"), None), P(None, "tp"), P(None, "tp"), P("tp", None)),
        out_specs=P(("dp", "tp"), None),
        check_vma=False,
    )
```
